32 devices in a mesh: gx: 4 (over y, core), gy: 4 (over z), gz: 2 (over x).
Axes of the slice: x: 2, y: 2, z: 4, core: 2. Of those that a mesh axis runs over, the one named last changes fastest.
Arguments:
- positions: float32 [3, 4, 32, 2, 128], P(None, 'gx', ('gy', 'gz')), may hold values from 0 to 3
- velocities: float32 [3, 4, 32, 2, 128], P(None, 'gx', ('gy', 'gz')), may hold values from -6 to 6
- bead_keys: int32 [4, 32, 2, 128], P('gx', ('gy', 'gz')), may hold values from 0 to 1073741823
- counts: int32 [4, 32, 2], P('gx', ('gy', 'gz')), may hold values from 64 to 128
Outputs:
- half_kick: float32 [3, 4, 32, 2, 128], P(None, 'gx', 'gy', 'gz')
The draws below stay inside these ranges and needn't reach their ends.
Inputs may be any that keep to these rules, and one draw needn't show every extreme that they name: Slots from counts of a tile on are padding and take no part. `bead_keys`: the lowest bit of a key names the bead type, 0 water and 1 polymer.
All inputs are finite; a program needn't handle non-finite values.
Results may differ from the reference program's by a relative error of at most 0.0003.
Values sent between devices are 32-bit elements; how exact they have to be, the bound alone decides.
No kernel may reach another device: no remote copies, remote signals or barrier semaphores. Data moves between devices by JAX's collectives and lax.ppermute only.
A program may use at most 64 MiB of HBM per device.

```python
import jax
import jax.numpy as jnp
from jax import lax

SLOTS = 128
SIDE = 3
NTX = 4
NTY = 32
NTZ = 2


def place_ends(values, own_key, smallest, top_value):
    index_at = [jax.random.randint(jax.random.fold_in(own_key, axis), (), 0, length) for axis, length in enumerate(values.shape)]
    main_axis = values.shape.index(max(values.shape))
    next_to = index_at[:main_axis] + [(index_at[main_axis] + 1) % values.shape[main_axis]] + index_at[main_axis + 1:]
    return values.at[tuple(index_at)].set(smallest).at[tuple(next_to)].set(top_value)


def levels(stream_key, shape, split, low, largest):
    def one(axis_at, blocks):
        heights = jax.random.uniform(jax.random.fold_in(jax.random.fold_in(stream_key, 6), axis_at), (blocks,), jnp.float32, low / len(split), largest / len(split))
        return jnp.repeat(jnp.exp(heights), shape[axis_at] // blocks).reshape((-1,) + (1,) * (len(shape) - axis_at - 1))

    factor_of = one(*split[0])
    for cut in split[1:]:
        factor_of = factor_of * one(*cut)
    return factor_of


def bell_draw(rng, extent, width, reach, split=(), kind=jnp.bfloat16):
    result = jax.random.normal(rng, extent, jnp.float32) * width
    if len(split) > 0:
        result = levels(rng, extent, split, -0.22, 0.18) * result
    return jnp.clip(result, min=-reach, max=reach).astype(kind)


def setup_inputs(seed: int = 0) -> dict:
    streams_of = jax.random.split(jax.random.key(seed), 5)
    return {
        "positions": jnp.clip(3.0 * jax.random.uniform(streams_of[0], (3, NTX, NTY, NTZ, SLOTS), jnp.float32) ** levels(streams_of[0], (3, NTX, NTY, NTZ, SLOTS), ((1, 4), (2, 8)), -0.2, 0.2), 0.0, 3.0),
        "velocities": bell_draw(streams_of[1], (3, NTX, NTY, NTZ, SLOTS), 1.0, 6.0, ((1, 4), (2, 8)), jnp.float32),
        "bead_keys": place_ends(jax.random.randint(streams_of[2], (NTX, NTY, NTZ, SLOTS), 0, 1073741824), jax.random.fold_in(streams_of[2], 1), 0, 1073741823).astype(jnp.int32),
        "counts": place_ends(jax.random.randint(streams_of[3], (NTX, NTY, NTZ), SLOTS // 2, SLOTS + 1), jax.random.fold_in(streams_of[3], 1), SLOTS // 2, SLOTS).astype(jnp.int32),
    }


soft_radius = 0.05
friction = 4.5
noise_amplitude = 15.0
like_repulsion = 25.0
unlike_extra = 15.0
kick_scale = 0.02
root_twelve = 3.4641016151377544

def pair_noise(first_keys, second_keys):
    hashed = (first_keys ^ second_keys) * 1103515245 + (first_keys + second_keys) * 12345
    hashed = hashed ^ hashed >> 15 & 131071
    hashed = hashed * 747796405
    hashed = hashed ^ hashed >> 13 & 524287
    fraction = (hashed >> 7 & 16777215).astype(jnp.float32) * (1.0 / 16777216.0)
    return root_twelve * (fraction - 0.5)

def pair_forces(own_motion, own_keys, other_motion, other_keys, other_counts, displace):
    slot_index = lax.broadcasted_iota(jnp.int32, other_keys.shape, 1)
    present = (slot_index < other_counts[:, None]).astype(jnp.float32)
    separation = [own_motion[component][:, :, None] - (other_motion[component][:, None, :] + displace[component]) for component in range(3)]
    squared = separation[0] * separation[0] + separation[1] * separation[1] + separation[2] * separation[2]
    distance = jnp.sqrt(squared)
    weight = jnp.maximum(1.0 - distance, 0.0) * present[:, None, :]
    inverse = 1.0 / jnp.maximum(distance, soft_radius)
    approach = separation[0] * (own_motion[3][:, :, None] - other_motion[3][:, None, :])
    approach = approach + separation[1] * (own_motion[4][:, :, None] - other_motion[4][:, None, :])
    approach = approach + separation[2] * (own_motion[5][:, :, None] - other_motion[5][:, None, :])
    approach = approach * inverse
    first_keys = own_keys[:, :, None]
    second_keys = other_keys[:, None, :]
    random_pair = pair_noise(first_keys, second_keys)
    repulsion = like_repulsion + unlike_extra * ((first_keys ^ second_keys) & 1).astype(jnp.float32)
    strength = (repulsion * weight - friction * weight * weight * approach + noise_amplitude * weight * random_pair) * inverse
    return jnp.stack([lax.optimization_barrier(jnp.sum(strength * part, axis=2)) for part in separation])

def reference(positions, velocities, bead_keys, counts):
    motion = jnp.concatenate([positions, velocities], axis=0)
    size_x, size_y, size_z, slots = bead_keys.shape
    plane = size_y * size_z
    own_motion = jnp.moveaxis(motion, 1, 0).reshape(size_x, 6, plane, slots)
    own_keys = bead_keys.reshape(size_x, plane, slots)
    summed = jnp.zeros((size_x, 3, plane, slots), jnp.float32)
    for off_x in range(3):
        for off_y in range(3):
            for off_z in range(3):
                moved = (1 - off_x, 1 - off_y, 1 - off_z)
                other_motion = jnp.moveaxis(jnp.roll(motion, moved, axis=(1, 2, 3)), 1, 0).reshape(size_x, 6, plane, slots)
                other_keys = jnp.roll(bead_keys, moved, axis=(0, 1, 2)).reshape(size_x, plane, slots)
                other_counts = jnp.roll(counts, moved, axis=(0, 1, 2)).reshape(size_x, plane)
                displace = jnp.array([SIDE * (off_x - 1), SIDE * (off_y - 1), SIDE * (off_z - 1)], jnp.float32)

                def one_plane(items, displace=displace):
                    return pair_forces(items[0], items[1], items[2], items[3], items[4], displace)
                summed = summed + lax.map(one_plane, (own_motion, own_keys, other_motion, other_keys, other_counts))
    slot_index = lax.broadcasted_iota(jnp.int32, bead_keys.shape, 3)
    occupied = (slot_index < counts[:, :, :, None]).astype(jnp.float32)
    force = jnp.moveaxis(summed, 1, 0).reshape(3, size_x, size_y, size_z, slots)
    return kick_scale * force * occupied[None]
```

```python
import functools

import jax
import jax.numpy as jnp
from jax import lax
from jax.experimental import pallas as pl
from jax.experimental.pallas import tpu as pltpu
from jax.sharding import PartitionSpec as P

SIDE = 3
ROWS = 16
FIRST = 64
CHUNK = 32

soft_radius = 0.05
friction = 4.5
noise_amplitude = 15.0
like_repulsion = 25.0
unlike_extra = 15.0
kick_scale = 0.02
root_twelve = 3.4641016151377544
FAR = 1.0e6
OCCUPIED = 1.0e5


def key_of(high, low):
    return (high.astype(jnp.int32) << 15) + low.astype(jnp.int32)


def pair_kernel(
    ymap, source, own, *rest, shifts, width, wraps, reach_y, size_z, final
):
    if final:
        own_counts, partial, out, mask, rank, pick, total, counts, pile, spread, own_keys, gathered = rest
    else:
        out, counts, mask, rank, pick, total, pile, spread, own_keys, gathered = rest
    slabs = len(shifts)
    stored_y = source.shape[1]
    slots = source.shape[4]
    tiles_per_slab = stored_y * width
    row = lax.broadcasted_iota(jnp.int32, (ROWS, slots), 0)
    off_y = row // 3 - 1
    off_z = row % 3 - 1

    def excess(place, off):
        part = jnp.where(off > 0, place, SIDE - place)
        return jnp.where(off == 0, 0.0, part * part)

    for slab in range(slabs):
        for y in range(stored_y):
            for z in range(width):
                place = source[slab, y, z]
                squared = excess(place[1:2], off_y) + excess(place[2:3], off_z)
                if shifts[slab] != 0:
                    edge = place[0:1] if shifts[slab] > 0 else SIDE - place[0:1]
                    squared = squared + edge * edge
                near = (squared < 1.00001) & (place[0:1] < OCCUPIED) & (row < 9)
                at = (slab * tiles_per_slab + y * width + z) * ROWS
                mask[at : at + ROWS] = jnp.where(near, 1.0, 0.0)
    chosen = mask[...].astype(jnp.bfloat16)
    before = lax.broadcasted_iota(jnp.int32, (slots, slots), 0)
    after = lax.broadcasted_iota(jnp.int32, (slots, slots), 1)
    upper = jnp.where(before <= after, 1.0, 0.0).astype(jnp.bfloat16)
    rank[...] = jnp.dot(chosen, upper, preferred_element_type=jnp.float32).astype(jnp.int32)
    ones = jnp.ones((8, slots), jnp.bfloat16)
    total[...] = lax.dot_general(
        ones, chosen, (((1,), (1,)), ((), ())), preferred_element_type=jnp.float32
    ).astype(jnp.int32)
    pltpu.sync_copy(total.at[pl.ds(0, 1)], counts)

    wanted = lax.broadcasted_iota(jnp.int32, rank.shape, 1)
    ranks = rank[...]
    found = jnp.zeros(rank.shape, jnp.int32)
    step = slots // 2
    while step:
        probe = jnp.take_along_axis(ranks, found + (step - 1), axis=1)
        found = found + jnp.where(probe <= wanted, step, 0)
        step //= 2
    pick[...] = found

    lane8 = lax.broadcasted_iota(jnp.int32, (8, slots), 1)
    row8 = lax.broadcasted_iota(jnp.int32, (8, slots), 0)
    far = jnp.where(row8 < 3, FAR, 0.0)
    tiles = reach_y * size_z

    def stored_z(halo_z):
        return lax.rem(halo_z, width) if wraps else halo_z

    def one_tile(t, carry):
        ty = t // size_z
        tz = t % size_z
        position = jnp.int32(0)
        current = far
        for slab in range(slabs):
            for oy in range(3):
                y = ymap[ty + oy]
                for oz in range(3):
                    z = stored_z(tz + oz)
                    at = slab * tiles_per_slab + y * width + z
                    which = oy * 3 + oz
                    index = jnp.broadcast_to(pick[pl.ds(at * ROWS + which, 1), :], (8, slots))
                    taken = jnp.take_along_axis(source[slab, y, z], index, axis=1)
                    shift = jnp.where(
                        row8 == 0,
                        float(SIDE * shifts[slab]),
                        jnp.where(
                            row8 == 1, float(SIDE * (oy - 1)), float(SIDE * (oz - 1))
                        ),
                    )
                    taken = taken + jnp.where(row8 < 3, shift, 0.0)
                    number = counts[0, at * ROWS + which]
                    start = position & (slots - 1)
                    rolled = pltpu.roll(taken, start, 1)
                    merged = jnp.where(lane8 >= start, rolled, current)
                    pile[position // slots] = merged
                    crossed = start + number >= slots
                    current = jnp.where(crossed, rolled, merged)
                    position = position + number
        left = position & (slots - 1)
        pile[position // slots] = jnp.where(lane8 < left, current, far)
        blocks = (position + (slots - 1)) // slots

        y_own = ymap[ty + 1]
        z_own = stored_z(tz + 1)
        own_block = own[y_own, z_own]
        if final:
            amount = own_counts[0, (y_own * width + z_own) * ROWS + 4]
        else:
            amount = counts[0, (y_own * width + z_own) * ROWS + 4]
        turned = jnp.transpose(own_block)
        for feature in range(6):
            spread[feature] = jnp.broadcast_to(turned[:, feature : feature + 1], (slots, slots))
        own_key = key_of(turned[:, 6:7], turned[:, 7:8])
        own_keys[...] = jnp.broadcast_to(own_key, (slots, slots))

        def rows_chunk(begin, rows):
            def add_block(b, summed):
                other = pile[b]

                def apart(feature):
                    mine = spread[feature, pl.ds(begin, rows), :]
                    return mine - other[feature : feature + 1]

                sep = [apart(c) for c in range(3)]
                speed = [apart(c + 3) for c in range(3)]
                squared = sep[0] * sep[0] + sep[1] * sep[1] + sep[2] * sep[2]
                root = lax.rsqrt(jnp.maximum(squared, 1e-30))
                weight = jnp.maximum(1.0 - squared * root, 0.0)
                inverse = jnp.minimum(root, 1.0 / soft_radius)
                approach = sep[0] * speed[0] + sep[1] * speed[1] + sep[2] * speed[2]
                first = own_keys[pl.ds(begin, rows), :]
                second = key_of(other[6:7], other[7:8])
                mixed = first ^ second
                hashed = mixed * 1103515245 + (first * 12345 + second * 12345)
                hashed = hashed ^ lax.shift_right_logical(hashed, 15)
                hashed = hashed * 747796405
                hashed = hashed ^ lax.shift_right_logical(hashed, 13)
                fraction = ((hashed >> 7) & 16777215).astype(jnp.float32)
                random_pair = fraction * (noise_amplitude * root_twelve / 16777216.0)
                low = like_repulsion - 0.5 * noise_amplitude * root_twelve
                level = jnp.where((mixed & 1) == 0, low, low + unlike_extra)
                strength = (
                    (random_pair + level - (friction * weight) * (approach * inverse))
                    * (weight * inverse)
                )
                return tuple(s + strength * part for s, part in zip(summed, sep))

            zero = jnp.zeros((rows, slots), jnp.float32)
            summed = lax.fori_loop(0, blocks, add_block, (zero, zero, zero))
            for c in range(3):
                gathered[c, pl.ds(begin, rows), :] = summed[c]

        rows_chunk(0, FIRST)

        def more(k, carry):
            rows_chunk(pl.multiple_of(FIRST + k * CHUNK, CHUNK), CHUNK)
            return carry

        lax.fori_loop(0, (amount - FIRST + CHUNK - 1) // CHUNK, more, 0)
        for c in range(3):
            force = jnp.sum(jnp.transpose(gathered[c]), axis=0, keepdims=True)
            if final:
                force = force + partial[c, pl.ds(t, 1), :]
                occupied = own_block[0:1] < OCCUPIED
                force = jnp.where(occupied, kick_scale * force, 0.0)
            out[c, pl.ds(t, 1), :] = force
        return carry

    lax.fori_loop(0, tiles, one_tile, 0)


def pair_call(ymap, source, own, earlier, *, shifts, wraps, reach_y, size_z):
    slabs, stored_y, width, _, slots = source.shape
    tiles = reach_y * size_z
    listed = slabs * stored_y * width * ROWS
    final = earlier is not None
    smem = pl.BlockSpec(memory_space=pltpu.SMEM)
    vmem = pl.BlockSpec(memory_space=pltpu.VMEM)
    force = jax.ShapeDtypeStruct((3, tiles, slots), jnp.float32)
    counted = (1, listed)
    common = [
        pltpu.VMEM((listed, slots), jnp.float32),
        pltpu.VMEM((listed, slots), jnp.int32),
        pltpu.VMEM((listed, slots), jnp.int32),
        pltpu.VMEM((8, listed), jnp.int32),
    ]
    tail = [
        pltpu.VMEM((slabs * 9 + 1, 8, slots), jnp.float32),
        pltpu.VMEM((6, slots, slots), jnp.float32),
        pltpu.VMEM((slots, slots), jnp.int32),
        pltpu.VMEM((3, slots, slots), jnp.float32),
    ]
    body = functools.partial(
        pair_kernel,
        shifts=shifts,
        width=width,
        wraps=wraps,
        reach_y=reach_y,
        size_z=size_z,
        final=final,
    )
    if final:
        return pl.pallas_call(
            body,
            out_shape=force,
            in_specs=[smem, vmem, vmem, smem, vmem],
            out_specs=vmem,
            scratch_shapes=common + [pltpu.SMEM(counted, jnp.int32)] + tail,
        )(ymap, source, own, *earlier)
    return pl.pallas_call(
        body,
        out_shape=(force, jax.ShapeDtypeStruct(counted, jnp.int32)),
        in_specs=[smem, vmem, vmem],
        out_specs=(vmem, smem),
        scratch_shapes=common + tail,
    )(ymap, source, own)


def gather_columns(packed, size_y, size_z, width):
    G, GY = lax.axis_size("gz"), lax.axis_size("gy")
    gz = lax.axis_index("gz")
    nz = packed.shape[2]
    twice = jnp.concatenate([packed, packed], axis=2)

    def piece(target, values):
        start = lax.rem(size_z * target - 1 + nz, nz)
        return lax.dynamic_slice_in_dim(values, start, width, axis=2)

    parts = [piece(gz, twice)]
    for delta in range(1, G):
        pairs = [(s, (s + delta) % G) for s in range(G)]
        parts.append(lax.ppermute(piece(lax.rem(gz + delta, G), twice), "gz", pairs))
    first, last = twice[:, :1], twice[:, size_y - 1 : size_y]
    ups, downs = [], []
    for k in range(G):
        ups.append([(y * G + G - 1, (y + 1) % GY * G + k) for y in range(GY)])
        downs.append([(y * G, (y - 1) % GY * G + (G - 1 - k)) for y in range(GY)])
    if G % 2 == 0:
        for k in range(G):
            upward = gz == G - 1
            layer = jnp.where(upward, last, first)
            payload = piece(jnp.where(upward, k, G - 1 - k), layer)
            parts.append(lax.ppermute(payload, ("gy", "gz"), ups[k] + downs[k]))
        low, high = gz, G - 1 - gz
    else:
        for k in range(G):
            parts.append(lax.ppermute(piece(jnp.int32(k), last), ("gy", "gz"), ups[k]))
        for k in range(G):
            parts.append(lax.ppermute(piece(jnp.int32(G - 1 - k), first), ("gy", "gz"), downs[k]))
        low, high = gz, 2 * G - 1 - gz
    base = size_y * G
    where = jnp.arange(base, dtype=jnp.int32)
    inner = lax.rem(gz - where // size_y + G, G) * size_y + where % size_y
    ymap = jnp.concatenate([(base + low)[None], inner, (base + high)[None]]).astype(jnp.int32)
    return jnp.concatenate(parts, axis=1), ymap


def on_device(positions, velocities, bead_keys, counts):
    lx, ly, nz, slots = bead_keys.shape
    G, GX = lax.axis_size("gz"), lax.axis_size("gx")
    size_z = nz // G
    width = min(size_z + 2, nz)
    reach_y = ly * G
    slot = lax.broadcasted_iota(jnp.int32, bead_keys.shape, 3)
    places = jnp.where((slot < counts[..., None])[None], positions, FAR)
    halves = jnp.stack([bead_keys >> 15, bead_keys & 32767]).astype(jnp.float32)
    packed = jnp.concatenate([places, velocities, halves], axis=0)
    packed = jnp.transpose(packed, (1, 2, 3, 0, 4))
    slab, ymap = gather_columns(packed, ly, size_z, width)
    up = [(i, (i + 1) % GX) for i in range(GX)]
    down = [(j, i) for i, j in up]
    below = lax.ppermute(slab[lx - 1 :], "gx", up)
    above = lax.ppermute(slab[:1], "gx", down)
    kicks = []
    sizes = dict(wraps=width == nz, reach_y=reach_y, size_z=size_z)
    for x in range(lx):
        own = slab[x]
        earlier = pair_call(ymap, slab[x : x + 1], own, None, shifts=(0,), **sizes)
        left = below if x == 0 else slab[x - 1 : x]
        right = above if x == lx - 1 else slab[x + 1 : x + 2]
        sides = jnp.concatenate([left, right], axis=0)
        earlier = (earlier[1], earlier[0])
        kicks.append(pair_call(ymap, sides, own, earlier, shifts=(-1, 1), **sizes))
    return jnp.stack(kicks, axis=1).reshape(3, lx, reach_y, size_z, slots)


def solution(mesh):
    in_specs = (
        P(None, "gx", ("gy", "gz"), None, None),
        P(None, "gx", ("gy", "gz"), None, None),
        P("gx", ("gy", "gz"), None, None),
        P("gx", ("gy", "gz"), None),
    )
    out_specs = P(None, "gx", "gy", "gz", None)
    return jax.shard_map(
        on_device, mesh=mesh, in_specs=in_specs, out_specs=out_specs, check_vma=False
    )
```

```python
import functools

import jax
import jax.numpy as jnp
from jax import lax
from jax.experimental import pallas as pl
from jax.experimental.pallas import tpu as pltpu
from jax.sharding import PartitionSpec as P

SIDE = 3
FIRST = 64
CHUNK = 32

soft_radius = 0.05
friction = 4.5
noise_amplitude = 15.0
like_repulsion = 25.0
unlike_extra = 15.0
kick_scale = 0.02
root_twelve = 3.4641016151377544
FAR = 1.0e6
OCCUPIED = 1.0e5


def key_of(high, low):
    return (high.astype(jnp.int32) << 15) + low.astype(jnp.int32)


def pair_kernel(
    column, *rest, slabs, shifts, width, wraps, size_y, edges, reach_y, size_z, final
):
    sources, rest = rest[:slabs], rest[slabs:]
    if final:
        own, own_counts, partial, out, mask, pick, total, counts, *rest = rest
    else:
        own = sources[0]
        out, counts, mask, pick, total, *rest = rest
    pile, spread, own_keys, gathered = rest
    slots = own.shape[-1]
    tiles = reach_y * size_z
    listed = mask.shape[0]
    gz = column[0]
    blocks_y = reach_y // size_y
    offsets = [(s, oy, oz) for s in range(slabs) for oy in range(3) for oz in range(3)]

    def stored_y(halo_y):
        if halo_y == 0:
            return reach_y + gz
        if halo_y > reach_y:
            return reach_y + edges - 1 - gz
        block, inner = divmod(halo_y - 1, size_y)
        delta = gz - block
        delta = jnp.where(delta < 0, delta + blocks_y, delta)
        return delta * size_y + inner

    def stored_z(halo_z):
        return halo_z % width if wraps else halo_z

    rows_y = [stored_y(h) for h in range(reach_y + 2)]

    def tile_at(t, offset):
        slab, oy, oz = offset
        return slab, rows_y[t // size_z + oy], stored_z(t % size_z + oz)

    if tiles * len(offsets) < listed:
        extra = listed - tiles * len(offsets)
        mask[tiles * len(offsets) :] = jnp.zeros((extra, slots), jnp.float32)
    for t in range(tiles):
        for n, offset in enumerate(offsets):
            slab, y, z = tile_at(t, offset)
            squared = None
            for axis, off in enumerate((shifts[slab], offset[1] - 1, offset[2] - 1)):
                if off != 0:
                    edge = sources[slab][0, y, z, axis : axis + 1, :]
                    edge = edge if off > 0 else SIDE - edge
                    squared = edge * edge if squared is None else squared + edge * edge
            if squared is None:
                near = sources[slab][0, y, z, 0:1, :] < OCCUPIED
            else:
                near = squared < 1.00001
            at = t * len(offsets) + n
            mask[at : at + 1] = jnp.where(near, 1.0, 0.0)
    chosen = mask[...].astype(jnp.bfloat16)
    ones = jnp.ones((8, slots), jnp.bfloat16)
    total[...] = lax.dot_general(
        ones, chosen, (((1,), (1,)), ((), ())), preferred_element_type=jnp.float32
    ).astype(jnp.int32)

    def send(semaphore):
        copy = pltpu.make_async_copy(total.at[pl.ds(0, 1)], counts, semaphore)
        copy.start()
        before = lax.broadcasted_iota(jnp.int32, (slots, slots), 0)
        after = lax.broadcasted_iota(jnp.int32, (slots, slots), 1)
        upper = jnp.where(before <= after, 1.0, 0.0).astype(jnp.bfloat16)
        ranks = jnp.dot(chosen, upper, preferred_element_type=jnp.float32).astype(jnp.int32)
        wanted = lax.broadcasted_iota(jnp.int32, (listed, slots), 1)
        found = jnp.zeros((listed, slots), jnp.int32)
        step = slots // 2
        while step:
            probe = jnp.take_along_axis(ranks, found + (step - 1), axis=1)
            found = found + jnp.where(probe <= wanted, step, 0)
            step //= 2
        pick[...] = found
        for t in range(tiles):
            _, y, z = tile_at(t, (0, 1, 1))
            turned = jnp.transpose(own[0, y, z])
            for feature in range(6):
                spread[t, feature] = jnp.broadcast_to(
                    turned[:, feature : feature + 1], (slots, slots)
                )
            own_key = key_of(turned[:, 6:7], turned[:, 7:8])
            own_keys[t] = jnp.broadcast_to(own_key, (slots, slots))
        copy.wait()

    pl.run_scoped(send, pltpu.SemaphoreType.DMA(()))

    lane8 = lax.broadcasted_iota(jnp.int32, (8, slots), 1)
    row8 = lax.broadcasted_iota(jnp.int32, (8, slots), 0)
    far = jnp.where(row8 < 3, FAR, 0.0)
    positions = [jnp.int32(0)] * tiles
    currents = [far] * tiles
    for n, offset in enumerate(offsets):
        shift = jnp.where(
            row8 == 0,
            float(SIDE * shifts[offset[0]]),
            jnp.where(row8 == 1, float(SIDE * (offset[1] - 1)), float(SIDE * (offset[2] - 1))),
        )
        shift = jnp.where(row8 < 3, shift, 0.0)
        for t in range(tiles):
            slab, y, z = tile_at(t, offset)
            at = t * len(offsets) + n
            index = jnp.broadcast_to(pick[at : at + 1, :], (8, slots))
            taken = jnp.take_along_axis(sources[slab][0, y, z], index, axis=1) + shift
            number = counts[0, at]
            start = positions[t] & (slots - 1)
            rolled = pltpu.roll(taken, start, 1)
            merged = jnp.where(lane8 >= start, rolled, currents[t])
            pile[t, positions[t] // slots] = merged
            currents[t] = jnp.where(start + number >= slots, rolled, merged)
            positions[t] = positions[t] + number
    for t in range(tiles):
        left = positions[t] & (slots - 1)
        pile[t, positions[t] // slots] = jnp.where(lane8 < left, currents[t], far)

    for t in range(tiles):
        blocks = (positions[t] + (slots - 1)) // slots
        if final:
            amount = own_counts[0, t * 9 + 4]
        else:
            amount = counts[0, t * 9 + 4]

        def rows_chunk(begin, rows, t=t, blocks=blocks):
            def add_block(b, summed):
                other = pile[t, b]

                def apart(feature):
                    mine = spread[t, feature, pl.ds(begin, rows), :]
                    return mine - other[feature : feature + 1]

                sep = [apart(c) for c in range(3)]
                speed = [apart(c + 3) for c in range(3)]
                squared = sep[0] * sep[0] + sep[1] * sep[1] + sep[2] * sep[2]
                root = lax.rsqrt(jnp.maximum(squared, 1e-30))
                weight = jnp.maximum(1.0 - squared * root, 0.0)
                inverse = jnp.minimum(root, 1.0 / soft_radius)
                approach = sep[0] * speed[0] + sep[1] * speed[1] + sep[2] * speed[2]
                first = own_keys[t, pl.ds(begin, rows), :]
                second = key_of(other[6:7], other[7:8])
                mixed = first ^ second
                hashed = mixed * 1103515245 + (first * 12345 + second * 12345)
                hashed = hashed ^ lax.shift_right_logical(hashed, 15)
                hashed = hashed * 747796405
                hashed = hashed ^ lax.shift_right_logical(hashed, 13)
                fraction = ((hashed >> 7) & 16777215).astype(jnp.float32)
                random_pair = fraction * (noise_amplitude * root_twelve / 16777216.0)
                low = like_repulsion - 0.5 * noise_amplitude * root_twelve
                level = jnp.where((mixed & 1) == 0, low, low + unlike_extra)
                strength = (
                    (random_pair + level - (friction * weight) * (approach * inverse))
                    * (weight * inverse)
                )
                return tuple(s + strength * part for s, part in zip(summed, sep))

            zero = jnp.zeros((rows, slots), jnp.float32)
            summed = lax.fori_loop(0, blocks, add_block, (zero, zero, zero))
            for c in range(3):
                gathered[t, c, pl.ds(begin, rows), :] = summed[c]

        rows_chunk(0, FIRST)

        def more(k, carry, rows_chunk=rows_chunk):
            rows_chunk(pl.multiple_of(FIRST + k * CHUNK, CHUNK), CHUNK)
            return carry

        lax.fori_loop(0, (amount - FIRST + CHUNK - 1) // CHUNK, more, 0)

    for t in range(tiles):
        _, y, z = tile_at(t, (0, 1, 1))
        for c in range(3):
            force = jnp.sum(jnp.transpose(gathered[t, c]), axis=0, keepdims=True)
            if final:
                force = force + partial[c, t : t + 1, :]
                occupied = own[0, y, z, 0:1, :] < OCCUPIED
                force = jnp.where(occupied, kick_scale * force, 0.0)
            out[c, t : t + 1, :] = force


def pair_call(column, sources, own, earlier, *, shifts, reach_y, size_z, **sizes):
    _, stored_y, width, _, slots = own.shape
    slabs = len(sources)
    tiles = reach_y * size_z
    listed = -(-tiles * slabs * 9 // 16) * 16
    final = earlier is not None
    smem = pl.BlockSpec(memory_space=pltpu.SMEM)
    vmem = pl.BlockSpec(memory_space=pltpu.VMEM)
    force = jax.ShapeDtypeStruct((3, tiles, slots), jnp.float32)
    counted = (1, listed)
    common = [
        pltpu.VMEM((listed, slots), jnp.float32),
        pltpu.VMEM((listed, slots), jnp.int32),
        pltpu.VMEM((8, listed), jnp.int32),
    ]
    tail = [
        pltpu.VMEM((tiles, slabs * 9 + 1, 8, slots), jnp.float32),
        pltpu.VMEM((tiles, 6, slots, slots), jnp.float32),
        pltpu.VMEM((tiles, slots, slots), jnp.int32),
        pltpu.VMEM((tiles, 3, slots, slots), jnp.float32),
    ]
    body = functools.partial(
        pair_kernel,
        slabs=slabs,
        shifts=shifts,
        width=width,
        reach_y=reach_y,
        size_z=size_z,
        final=final,
        **sizes,
    )
    if final:
        return pl.pallas_call(
            body,
            out_shape=force,
            in_specs=[smem] + [vmem] * (slabs + 1) + [smem, vmem],
            out_specs=vmem,
            scratch_shapes=common + [pltpu.SMEM(counted, jnp.int32)] + tail,
        )(column, *sources, own, *earlier)
    return pl.pallas_call(
        body,
        out_shape=(force, jax.ShapeDtypeStruct(counted, jnp.int32)),
        in_specs=[smem] + [vmem] * slabs,
        out_specs=(vmem, smem),
        scratch_shapes=common + tail,
    )(column, *sources)


def gather_columns(packed, size_y, size_z, width):
    G, GY = lax.axis_size("gz"), lax.axis_size("gy")
    gz = lax.axis_index("gz")
    nz = packed.shape[2]
    twice = jnp.concatenate([packed, packed], axis=2)

    def piece(target, values):
        start = lax.rem(size_z * target - 1 + nz, nz)
        return lax.dynamic_slice_in_dim(values, start, width, axis=2)

    parts = [piece(gz, twice)]
    for delta in range(1, G):
        pairs = [(s, (s + delta) % G) for s in range(G)]
        parts.append(lax.ppermute(piece(lax.rem(gz + delta, G), twice), "gz", pairs))
    first, last = twice[:, :1], twice[:, size_y - 1 : size_y]
    ups, downs = [], []
    for k in range(G):
        ups.append([(y * G + G - 1, (y + 1) % GY * G + k) for y in range(GY)])
        downs.append([(y * G, (y - 1) % GY * G + (G - 1 - k)) for y in range(GY)])
    if G % 2 == 0:
        for k in range(G):
            upward = gz == G - 1
            layer = jnp.where(upward, last, first)
            payload = piece(jnp.where(upward, k, G - 1 - k), layer)
            parts.append(lax.ppermute(payload, ("gy", "gz"), ups[k] + downs[k]))
    else:
        for k in range(G):
            parts.append(lax.ppermute(piece(jnp.int32(k), last), ("gy", "gz"), ups[k]))
        for k in range(G):
            parts.append(lax.ppermute(piece(jnp.int32(G - 1 - k), first), ("gy", "gz"), downs[k]))
    return jnp.concatenate(parts, axis=1)


def on_device(positions, velocities, bead_keys, counts):
    lx, ly, nz, slots = bead_keys.shape
    G, GX = lax.axis_size("gz"), lax.axis_size("gx")
    size_z = nz // G
    width = min(size_z + 2, nz)
    reach_y = ly * G
    slot = lax.broadcasted_iota(jnp.int32, bead_keys.shape, 3)
    places = jnp.where((slot < counts[..., None])[None], positions, FAR)
    halves = jnp.stack([bead_keys >> 15, bead_keys & 32767]).astype(jnp.float32)
    packed = jnp.concatenate([places, velocities, halves], axis=0)
    packed = jnp.transpose(packed, (1, 2, 3, 0, 4))
    slab = gather_columns(packed, ly, size_z, width)
    up = [(i, (i + 1) % GX) for i in range(GX)]
    down = [(j, i) for i, j in up]
    below = lax.ppermute(slab[lx - 1 :], "gx", up)
    above = lax.ppermute(slab[:1], "gx", down)
    kicks = []
    column = lax.axis_index("gz").astype(jnp.int32)[None]
    sizes = dict(
        wraps=width == nz,
        size_y=ly,
        edges=slab.shape[1] - reach_y,
        reach_y=reach_y,
        size_z=size_z,
    )
    for x in range(lx):
        own = slab[x : x + 1]
        partial, own_counts = pair_call(column, (own,), own, None, shifts=(0,), **sizes)
        left = below if x == 0 else slab[x - 1 : x]
        right = above if x == lx - 1 else slab[x + 1 : x + 2]
        earlier = (own_counts, partial)
        kicks.append(pair_call(column, (left, right), own, earlier, shifts=(-1, 1), **sizes))
    return jnp.stack(kicks, axis=1).reshape(3, lx, reach_y, size_z, slots)


def solution(mesh):
    in_specs = (
        P(None, "gx", ("gy", "gz"), None, None),
        P(None, "gx", ("gy", "gz"), None, None),
        P("gx", ("gy", "gz"), None, None),
        P("gx", ("gy", "gz"), None),
    )
    out_specs = P(None, "gx", "gy", "gz", None)
    return jax.shard_map(
        on_device, mesh=mesh, in_specs=in_specs, out_specs=out_specs, check_vma=False
    )
```

```python
import functools

import jax
import jax.numpy as jnp
from jax import lax
from jax.experimental import pallas as pl
from jax.experimental.pallas import tpu as pltpu
from jax.sharding import PartitionSpec as P

SIDE = 3
FIRST = 64
CHUNK = 32

soft_radius = 0.05
friction = 4.5
noise_amplitude = 15.0
like_repulsion = 25.0
unlike_extra = 15.0
kick_scale = 0.02
root_twelve = 3.4641016151377544
FAR = 1.0e6
OCCUPIED = 1.0e5


def key_of(high, low):
    return (high.astype(jnp.int32) << 15) + low.astype(jnp.int32)


def pair_kernel(
    column, *rest, slabs, shifts, width, wraps, size_y, edges, reach_y, size_z, final
):
    sources, rest = rest[:slabs], rest[slabs:]
    if final:
        own_total, partial, carried, out, mask, pick, total, counts, own_counts, *rest = rest
    else:
        out, total, carried, mask, pick, counts, *rest = rest
    pile, spread, own_keys, gathered = rest
    slots = sources[0].shape[-1]
    tiles = reach_y * size_z
    listed = mask.shape[0]
    gz = column[0]
    blocks_y = reach_y // size_y
    offsets = [(s, oy, oz) for s in range(slabs) for oy in range(3) for oz in range(3)]

    def stored_y(halo_y):
        if halo_y == 0:
            return reach_y + gz
        if halo_y > reach_y:
            return reach_y + edges - 1 - gz
        block, inner = divmod(halo_y - 1, size_y)
        delta = gz - block
        delta = jnp.where(delta < 0, delta + blocks_y, delta)
        return delta * size_y + inner

    def stored_z(halo_z):
        return halo_z % width if wraps else halo_z

    rows_y = [stored_y(h) for h in range(reach_y + 2)]

    def tile_at(t, offset):
        slab, oy, oz = offset
        return slab, rows_y[t // size_z + oy], stored_z(t % size_z + oz)

    if tiles * len(offsets) < listed:
        extra = listed - tiles * len(offsets)
        mask[tiles * len(offsets) :] = jnp.zeros((extra, slots), jnp.float32)
    for t in range(tiles):
        for n, offset in enumerate(offsets):
            slab, y, z = tile_at(t, offset)
            squared = None
            for axis, off in enumerate((shifts[slab], offset[1] - 1, offset[2] - 1)):
                if off != 0:
                    edge = sources[slab][0, y, z, axis : axis + 1, :]
                    edge = edge if off > 0 else SIDE - edge
                    squared = edge * edge if squared is None else squared + edge * edge
            if squared is None:
                near = sources[slab][0, y, z, 0:1, :] < OCCUPIED
            else:
                near = squared < 1.00001
            at = t * len(offsets) + n
            mask[at : at + 1] = jnp.where(near, 1.0, 0.0)
    chosen = mask[...].astype(jnp.bfloat16)
    ones = jnp.ones((8, slots), jnp.bfloat16)
    total[...] = lax.dot_general(
        ones, chosen, (((1,), (1,)), ((), ())), preferred_element_type=jnp.float32
    ).astype(jnp.int32)

    def send(semaphore, *own_semaphore):
        copy = pltpu.make_async_copy(total.at[pl.ds(0, 1)], counts, semaphore)
        copy.start()
        if final:
            own_copy = pltpu.make_async_copy(
                own_total.at[pl.ds(0, 1)], own_counts, own_semaphore[0]
            )
            own_copy.start()
        before = lax.broadcasted_iota(jnp.int32, (slots, slots), 0)
        after = lax.broadcasted_iota(jnp.int32, (slots, slots), 1)
        upper = jnp.where(before <= after, 1.0, 0.0).astype(jnp.bfloat16)
        ranks = jnp.dot(chosen, upper, preferred_element_type=jnp.float32).astype(jnp.int32)
        wanted = lax.broadcasted_iota(jnp.int32, (listed, slots), 1)
        found = jnp.zeros((listed, slots), jnp.int32)
        step = slots // 2
        while step:
            probe = jnp.take_along_axis(ranks, found + (step - 1), axis=1)
            found = found + jnp.where(probe <= wanted, step, 0)
            step //= 2
        pick[...] = found
        for t in range(tiles):
            if not final:
                _, y, z = tile_at(t, (0, 1, 1))
                carried[t, 1] = sources[0][0, y, z]
            turned = jnp.transpose(carried[t, 1])
            for feature in range(6):
                spread[t, feature] = jnp.broadcast_to(
                    turned[:, feature : feature + 1], (slots, slots)
                )
            own_key = key_of(turned[:, 6:7], turned[:, 7:8])
            own_keys[t] = jnp.broadcast_to(own_key, (slots, slots))
        copy.wait()
        if final:
            own_copy.wait()

    pl.run_scoped(send, *[pltpu.SemaphoreType.DMA(())] * (2 if final else 1))

    lane8 = lax.broadcasted_iota(jnp.int32, (8, slots), 1)
    row8 = lax.broadcasted_iota(jnp.int32, (8, slots), 0)
    far = jnp.where(row8 < 3, FAR, 0.0)
    positions = [jnp.int32(0)] * tiles
    currents = [far] * tiles
    if final:
        for t in range(tiles):
            listed_before = own_counts[0, t * 9]
            for n in range(1, 9):
                listed_before = listed_before + own_counts[0, t * 9 + n]
            positions[t] = listed_before & (slots - 1)
            currents[t] = carried[t, 0]
    for n, offset in enumerate(offsets):
        shift = jnp.where(
            row8 == 0,
            float(SIDE * shifts[offset[0]]),
            jnp.where(row8 == 1, float(SIDE * (offset[1] - 1)), float(SIDE * (offset[2] - 1))),
        )
        shift = jnp.where(row8 < 3, shift, 0.0)
        for t in range(tiles):
            slab, y, z = tile_at(t, offset)
            at = t * len(offsets) + n
            index = jnp.broadcast_to(pick[at : at + 1, :], (8, slots))
            taken = jnp.take_along_axis(sources[slab][0, y, z], index, axis=1) + shift
            number = counts[0, at]
            start = positions[t] & (slots - 1)
            rolled = pltpu.roll(taken, start, 1)
            merged = jnp.where(lane8 >= start, rolled, currents[t])
            pile[t, positions[t] // slots] = merged
            currents[t] = jnp.where(start + number >= slots, rolled, merged)
            positions[t] = positions[t] + number
    for t in range(tiles):
        if final:
            left = positions[t] & (slots - 1)
            pile[t, positions[t] // slots] = jnp.where(lane8 < left, currents[t], far)
        else:
            carried[t, 0] = currents[t]

    for t in range(tiles):
        blocks = (positions[t] + (slots - 1 if final else 0)) // slots
        if final:
            amount = own_counts[0, t * 9 + 4]
        else:
            amount = counts[0, t * 9 + 4]

        def rows_chunk(begin, rows, t=t, blocks=blocks):
            def add_block(b, summed):
                other = pile[t, b]

                def apart(feature):
                    mine = spread[t, feature, pl.ds(begin, rows), :]
                    return mine - other[feature : feature + 1]

                sep = [apart(c) for c in range(3)]
                speed = [apart(c + 3) for c in range(3)]
                squared = sep[0] * sep[0] + sep[1] * sep[1] + sep[2] * sep[2]
                root = lax.rsqrt(jnp.maximum(squared, 1e-30))
                weight = jnp.maximum(1.0 - squared * root, 0.0)
                inverse = jnp.minimum(root, 1.0 / soft_radius)
                approach = sep[0] * speed[0] + sep[1] * speed[1] + sep[2] * speed[2]
                first = own_keys[t, pl.ds(begin, rows), :]
                second = key_of(other[6:7], other[7:8])
                mixed = first ^ second
                hashed = mixed * 1103515245 + (first * 12345 + second * 12345)
                hashed = hashed ^ lax.shift_right_logical(hashed, 15)
                hashed = hashed * 747796405
                hashed = hashed ^ lax.shift_right_logical(hashed, 13)
                fraction = ((hashed >> 7) & 16777215).astype(jnp.float32)
                random_pair = fraction * (noise_amplitude * root_twelve / 16777216.0)
                low = like_repulsion - 0.5 * noise_amplitude * root_twelve
                level = jnp.where((mixed & 1) == 0, low, low + unlike_extra)
                strength = (
                    (random_pair + level - (friction * weight) * (approach * inverse))
                    * (weight * inverse)
                )
                return tuple(s + strength * part for s, part in zip(summed, sep))

            zero = jnp.zeros((rows, slots), jnp.float32)
            summed = lax.fori_loop(0, blocks, add_block, (zero, zero, zero))
            for c in range(3):
                gathered[t, c, pl.ds(begin, rows), :] = summed[c]

        rows_chunk(0, FIRST)

        def more(k, carry, rows_chunk=rows_chunk):
            rows_chunk(pl.multiple_of(FIRST + k * CHUNK, CHUNK), CHUNK)
            return carry

        lax.fori_loop(0, (amount - FIRST + CHUNK - 1) // CHUNK, more, 0)

    for t in range(tiles):
        for c in range(3):
            force = jnp.sum(jnp.transpose(gathered[t, c]), axis=0, keepdims=True)
            if final:
                force = force + partial[c, t : t + 1, :]
                occupied = carried[t, 1, 0:1, :] < OCCUPIED
                force = jnp.where(occupied, kick_scale * force, 0.0)
            out[c, t : t + 1, :] = force


def pair_call(column, sources, earlier, *, shifts, reach_y, size_z, **sizes):
    _, _, width, _, slots = sources[0].shape
    slabs = len(sources)
    tiles = reach_y * size_z
    listed = -(-tiles * slabs * 9 // 16) * 16
    final = earlier is not None
    smem = pl.BlockSpec(memory_space=pltpu.SMEM)
    vmem = pl.BlockSpec(memory_space=pltpu.VMEM)
    force = jax.ShapeDtypeStruct((3, tiles, slots), jnp.float32)
    counted = (1, listed)
    common = [
        pltpu.VMEM((listed, slots), jnp.float32),
        pltpu.VMEM((listed, slots), jnp.int32),
    ]
    tail = [
        pltpu.VMEM((tiles, slabs * 9 + 2, 8, slots), jnp.float32),
        pltpu.VMEM((tiles, 6, slots, slots), jnp.float32),
        pltpu.VMEM((tiles, slots, slots), jnp.int32),
        pltpu.VMEM((tiles, 3, slots, slots), jnp.float32),
    ]
    body = functools.partial(
        pair_kernel,
        slabs=slabs,
        shifts=shifts,
        width=width,
        reach_y=reach_y,
        size_z=size_z,
        final=final,
        **sizes,
    )
    if final:
        return pl.pallas_call(
            body,
            out_shape=force,
            in_specs=[smem] + [vmem] * (slabs + 3),
            out_specs=vmem,
            scratch_shapes=common
            + [
                pltpu.VMEM((8, listed), jnp.int32),
                pltpu.SMEM(counted, jnp.int32),
                pltpu.SMEM((1, earlier[0].shape[1]), jnp.int32),
            ]
            + tail,
        )(column, *sources, *earlier)
    return pl.pallas_call(
        body,
        out_shape=(
            force,
            jax.ShapeDtypeStruct((8, listed), jnp.int32),
            jax.ShapeDtypeStruct((tiles, 2, 8, slots), jnp.float32),
        ),
        in_specs=[smem] + [vmem] * slabs,
        out_specs=(vmem, vmem, vmem),
        scratch_shapes=common + [pltpu.SMEM(counted, jnp.int32)] + tail,
    )(column, *sources)


def gather_columns(packed, size_y, size_z, width):
    G, GY = lax.axis_size("gz"), lax.axis_size("gy")
    gz = lax.axis_index("gz")
    nz = packed.shape[2]
    twice = jnp.concatenate([packed, packed], axis=2)

    def piece(target, values):
        start = lax.rem(size_z * target - 1 + nz, nz)
        return lax.dynamic_slice_in_dim(values, start, width, axis=2)

    parts = [piece(gz, twice)]
    for delta in range(1, G):
        pairs = [(s, (s + delta) % G) for s in range(G)]
        parts.append(lax.ppermute(piece(lax.rem(gz + delta, G), twice), "gz", pairs))
    first, last = twice[:, :1], twice[:, size_y - 1 : size_y]
    ups, downs = [], []
    for k in range(G):
        ups.append([(y * G + G - 1, (y + 1) % GY * G + k) for y in range(GY)])
        downs.append([(y * G, (y - 1) % GY * G + (G - 1 - k)) for y in range(GY)])
    if G % 2 == 0:
        for k in range(G):
            upward = gz == G - 1
            layer = jnp.where(upward, last, first)
            payload = piece(jnp.where(upward, k, G - 1 - k), layer)
            parts.append(lax.ppermute(payload, ("gy", "gz"), ups[k] + downs[k]))
    else:
        for k in range(G):
            parts.append(lax.ppermute(piece(jnp.int32(k), last), ("gy", "gz"), ups[k]))
        for k in range(G):
            parts.append(lax.ppermute(piece(jnp.int32(G - 1 - k), first), ("gy", "gz"), downs[k]))
    return jnp.concatenate(parts, axis=1)


def on_device(positions, velocities, bead_keys, counts):
    lx, ly, nz, slots = bead_keys.shape
    G, GX = lax.axis_size("gz"), lax.axis_size("gx")
    size_z = nz // G
    width = min(size_z + 2, nz)
    reach_y = ly * G
    slot = lax.broadcasted_iota(jnp.int32, bead_keys.shape, 3)
    places = jnp.where((slot < counts[..., None])[None], positions, FAR)
    halves = jnp.stack([bead_keys >> 15, bead_keys & 32767]).astype(jnp.float32)
    packed = jnp.concatenate([places, velocities, halves], axis=0)
    packed = jnp.transpose(packed, (1, 2, 3, 0, 4))
    slab = gather_columns(packed, ly, size_z, width)
    up = [(i, (i + 1) % GX) for i in range(GX)]
    down = [(j, i) for i, j in up]
    below = lax.ppermute(slab[lx - 1 :], "gx", up)
    above = lax.ppermute(slab[:1], "gx", down)
    kicks = []
    column = lax.axis_index("gz").astype(jnp.int32)[None]
    sizes = dict(
        wraps=width == nz,
        size_y=ly,
        edges=slab.shape[1] - reach_y,
        reach_y=reach_y,
        size_z=size_z,
    )
    for x in range(lx):
        own = slab[x : x + 1]
        partial, own_total, carried = pair_call(column, (own,), None, shifts=(0,), **sizes)
        left = below if x == 0 else slab[x - 1 : x]
        right = above if x == lx - 1 else slab[x + 1 : x + 2]
        earlier = (own_total, partial, carried)
        kicks.append(pair_call(column, (left, right), earlier, shifts=(-1, 1), **sizes))
    return jnp.stack(kicks, axis=1).reshape(3, lx, reach_y, size_z, slots)


def solution(mesh):
    in_specs = (
        P(None, "gx", ("gy", "gz"), None, None),
        P(None, "gx", ("gy", "gz"), None, None),
        P("gx", ("gy", "gz"), None, None),
        P("gx", ("gy", "gz"), None),
    )
    out_specs = P(None, "gx", "gy", "gz", None)
    return jax.shard_map(
        on_device, mesh=mesh, in_specs=in_specs, out_specs=out_specs, check_vma=False
    )
```
